32 devices in a mesh: rep: 1, dp: 32 (over x, y, z, core).
Axes of the slice: x: 2, y: 2, z: 4, core: 2. Of those that a mesh axis runs over, the one named last changes fastest.
Arguments:
- a: bfloat16 [32, 2, 4096, 1024], P(('rep', 'dp'))
- g: bfloat16 [32, 2, 4096, 3200], P(('rep', 'dp'))
Outputs:
- output: bfloat16 [2, 1024, 3200], P('rep')
All inputs are finite; a program needn't handle non-finite values.
Results may differ from the reference program's by a relative error of at most 0.012.
Values are sent between devices in bfloat16 or wider.
A program may use at most 2 GiB of HBM per device.

```python
import jax
import jax.numpy as jnp
from jax import lax

DEVICES = 32
MATRICES = 2
TOKENS = 4096
D = 1024
FF = 3200


def setup_inputs(seed: int = 0, part: int = 0) -> dict:
    ka, kg, ks = (jax.random.fold_in(k, part) for k in jax.random.split(jax.random.key(seed), 3))
    size = 2.0 ** jax.random.uniform(ks, (DEVICES, MATRICES, 1, 1), jnp.float32, -1.0, 1.0)
    a = jax.random.normal(ka, (DEVICES, MATRICES, TOKENS, D), jnp.float32)
    g = size * jax.random.normal(kg, (DEVICES, MATRICES, TOKENS, FF), jnp.float32) * (DEVICES * TOKENS) ** -0.5
    return {"a": a.astype(jnp.bfloat16), "g": g.astype(jnp.bfloat16)}


def reference(a, g):
    def take(so_far, one):
        return so_far + jnp.einsum("ntd,ntf->ndf", *one, preferred_element_type=jnp.float32), None

    return lax.scan(take, jnp.zeros((MATRICES, D, FF), jnp.float32), (a, g))[0].astype(jnp.bfloat16)
```

```python
import functools

import jax
import jax.numpy as jnp
from jax import lax
from jax.experimental import pallas as pl
from jax.experimental.pallas import tpu as pltpu
from jax.sharding import PartitionSpec as P

W = 256
RING = 8
MESH = pl.DeviceIdType.MESH
F32, BF16 = jnp.float32, jnp.bfloat16
HOP = 2

O_D2D = 1
O_A = O_D2D + HOP
O_Z1, O_Z2, O_Z3 = O_A + HOP, O_A + 2 * HOP, O_A + 3 * HOP
O_B = O_Z3 + HOP
O_BG = O_B + HOP
O_ZG1, O_ZG2, O_ZG3 = O_BG + HOP, O_BG + 2 * HOP, O_BG + 3 * HOP
O_AG = O_ZG3 + HOP
O_DG = O_AG + 1
O_OUT = O_DG + 2
KEEP = O_B - O_D2D + 1


def kernel(full, a_hbm, g_hbm, out_hbm, a_v, g_v, acc, keep, res, d_send, d_recv, a_send, a_recv, zr_send, zr_recv, zl_send, zl_recv,
           b_send, b_recv, in_sem, out_sem, s_sem, r_sem, zs_sem, zr_sem):
    chunks = 2 * full + 1
    rows = acc.shape[1]
    half, quarter, block, piece = rows // 2, rows // 4, rows // 16, rows // 32
    me = lax.axis_index("dp")
    x, y, z, core = me // 16, (me // 8) % 2, (me // 2) % 4, me % 2

    def dev(x, y, z, core):
        return {"dp": ((x * 2 + y) * 4 + z) * 2 + core}

    partner = dev(x, y, z, 1 - core)
    first = 1 - core
    a_at = first * x + core * y
    b_at = first * y + core * x
    a_dev = dev(x + first * (1 - 2 * x), y + core * (1 - 2 * y), z, core)
    b_dev = dev(x + core * (1 - 2 * x), y + first * (1 - 2 * y), z, core)
    right, left = dev(x, y, z + 1, core), dev(x, y, z - 1, core)

    def at(start, size):
        return pl.ds(pl.multiple_of(start, size), size)

    def remote(src, dst, send, recv, to):
        return pltpu.make_async_remote_copy(src, dst, send, recv, device_id=to, device_id_type=MESH)

    def g_copies(i, slot):
        m = (i > full).astype(jnp.int32)
        start = pl.multiple_of((i - m * (full + 1)) * W, W)
        return pltpu.make_async_copy(g_hbm.at[0, m, :, pl.ds(start, W)], g_v.at[slot], in_sem.at[slot])

    def g_mixed(m, slot):
        return pltpu.make_async_copy(
            g_hbm.at[0, m, :, pl.ds(full * W, W // 2)], g_v.at[slot, :, pl.ds(m * (W // 2), W // 2)], in_sem.at[3 + m]
        )

    def g_start(i, slot):
        @pl.when(i != full)
        def _():
            g_copies(i, slot).start()

        @pl.when(i == full)
        def _():
            g_mixed(0, slot).start()
            g_mixed(1, slot).start()

    def a_copy(m):
        return pltpu.make_async_copy(a_hbm.at[0, m], a_v.at[m], in_sem.at[5 + m])

    a_copy(0).start()
    for i in range(3):
        g_start(jnp.int32(i), i)
    a_copy(1).start()

    barrier = pltpu.get_barrier_semaphore()
    for to in (partner, a_dev, b_dev):
        pl.semaphore_signal(barrier, inc=1, device_id=to, device_id_type=MESH)

    @pl.when(z < 3)
    def _():
        pl.semaphore_signal(barrier, inc=1, device_id=right, device_id_type=MESH)

    @pl.when(z > 0)
    def _():
        pl.semaphore_signal(barrier, inc=1, device_id=left, device_id_type=MESH)

    pl.semaphore_wait(barrier, 3 + (z < 3).astype(jnp.int32) + (z > 0).astype(jnp.int32))
    a_copy(0).wait()

    def pair(k, i, src, dst, to):
        s = lax.rem(i, RING)
        return remote(src, dst, s_sem.at[k, s], r_sem.at[k, s], to)

    def d_copy(i):
        s = lax.rem(i, RING)
        return pair(0, i, d_send.at[s], d_recv.at[s], partner)

    def a_copy_out(i):
        s = lax.rem(i, RING)
        return pair(1, i, a_send.at[s], a_recv.at[s], a_dev)

    def b_copy(i):
        s = lax.rem(i, RING)
        return pair(2, i, b_send.at[s], b_recv.at[s], b_dev)

    mine_a = core * half + a_at * quarter
    mine_z = mine_a + z * block
    mine_b = mine_z + b_at * piece

    def bg_copy(i):
        ref = res.at[i, at(mine_b, piece)]
        return pair(3, i, ref, ref, b_dev)

    def ag_copy(i):
        ref = res.at[i, at(mine_a, quarter)]
        return pair(4, i, ref, ref, a_dev)

    def dg_copy(i):
        ref = res.at[i, at(core * half, half)]
        return pair(5, i, ref, ref, partner)

    def z_copy(i, way, lo, hi):
        s = lax.rem(i, RING)
        send, recv, to = ((zr_send, zr_recv, right), (zl_send, zl_recv, left))[way]
        there = pl.ds(lo * block, (hi - lo) * block)
        return remote(send.at[s, there], recv.at[s, there], zs_sem.at[way, s], zr_sem.at[way, s], to)

    def zg_copy(i, way, hop):
        s = lax.rem(i, RING)
        owner = z - (hop - 1) if way == 0 else z + (hop - 1)
        ref = res.at[i, at(mine_a + owner * block, block)]
        k = 2 + way * 3 + hop - 1
        return remote(ref, ref, zs_sem.at[k, s], zr_sem.at[k, s], (right, left)[way])

    def stage(step, offset, body):
        i = step - offset

        @pl.when((i >= 0) & (i < chunks))
        def _():
            body(i)

    def multiply(i):
        slot = lax.rem(i, 3)
        now = lax.rem(i, 2)
        dims = (((0,), (0,)), ((), ()))

        @pl.when(i != full)
        def _():
            m = (i > full).astype(jnp.int32)

            g_copies(i, slot).wait()
            acc[now] = lax.dot_general(a_v[m], g_v[slot], dims, preferred_element_type=F32)

        @pl.when(i == full)
        def _():
            a_copy(1).wait()
            for m in range(2):
                g_mixed(m, slot).wait()
                part = pl.ds(m * (W // 2), W // 2)
                acc[now, :, part] = lax.dot_general(a_v[m], g_v[slot, :, part], dims, preferred_element_type=F32)

        @pl.when(i + 3 < chunks)
        def _():
            g_start(i + 3, slot)

        d_send[lax.rem(i, RING)] = acc[now, at((1 - core) * half, half)].astype(BF16)
        d_copy(i).start()

    def on_d2d(i):
        d_copy(i).wait()
        s, k, now = lax.rem(i, RING), lax.rem(i, KEEP), lax.rem(i, 2)

        def total(which):
            here = at(core * half + which * quarter, quarter)
            return acc[now, here] + d_recv[s, at(which * quarter, quarter)].astype(F32)

        a_send[s] = total(1 - a_at).astype(BF16)
        a_copy_out(i).start()
        keep[k] = total(a_at)

    def on_a(i):
        a_copy_out(i).wait()
        s, k = lax.rem(i, RING), lax.rem(i, KEEP)
        keep[k] += a_recv[s].astype(F32)

        @pl.when(z == 0)
        def _():
            there = pl.ds(block, 3 * block)
            zr_send[s, there] = keep[k, there].astype(BF16)
            z_copy(i, 0, 1, 4).start()

        @pl.when(z == 3)
        def _():
            there = pl.ds(0, 3 * block)
            zl_send[s, there] = keep[k, there].astype(BF16)
            z_copy(i, 1, 0, 3).start()

    def pass_on(i, way, at_z):
        s, k = lax.rem(i, RING), lax.rem(i, KEEP)
        send, recv = ((zr_send, zr_recv), (zl_send, zl_recv))[way]
        lo, hi = ((at_z, 4), (0, at_z + 1))[way]

        @pl.when(z == at_z)
        def _():
            z_copy(i, way, lo, hi).wait_recv()
            lo2, hi2 = ((at_z + 1, 4), (0, at_z))[way]
            if lo2 < hi2:
                beyond = pl.ds(lo2 * block, (hi2 - lo2) * block)
                send[s, beyond] = (keep[k, beyond] + recv[s, beyond].astype(F32)).astype(BF16)
                z_copy(i, way, lo2, hi2).start()
            here = pl.ds(at_z * block, block)
            keep[k, here] += recv[s, here].astype(F32)

    def sent(i, way, at_z):
        lo, hi = ((at_z + 1, 4), (0, at_z))[way]

        @pl.when(z == at_z)
        def _():
            z_copy(i, way, lo, hi).wait_send()

    def on_z1(i):
        sent(i, 0, 0)
        sent(i, 1, 3)
        pass_on(i, 0, 1)
        pass_on(i, 1, 2)

    def on_z2(i):
        sent(i, 0, 1)
        sent(i, 1, 2)
        pass_on(i, 0, 2)
        pass_on(i, 1, 1)

    def on_z3(i):
        sent(i, 0, 2)
        sent(i, 1, 1)
        pass_on(i, 0, 3)
        pass_on(i, 1, 0)
        s, k = lax.rem(i, RING), lax.rem(i, KEEP)
        b_send[s] = keep[k, at(z * block + (1 - b_at) * piece, piece)].astype(BF16)
        b_copy(i).start()

    def on_b(i):
        b_copy(i).wait()
        s, k = lax.rem(i, RING), lax.rem(i, KEEP)
        total = keep[k, at(z * block + b_at * piece, piece)] + b_recv[s].astype(F32)
        res[i, at(mine_b, piece)] = total.astype(BF16)
        bg_copy(i).start()

    def can(way, hop):
        return (z >= hop - 1) & (z < 3) if way == 0 else (z <= 4 - hop) & (z > 0)

    def gets(way, hop):
        return z >= hop if way == 0 else z <= 3 - hop

    def gather(i, hop):
        for way in range(2):
            if hop > 0:

                @pl.when(gets(way, hop))
                def _():
                    zg_copy(i, way, hop).wait_recv()

            if hop < 3:

                @pl.when(can(way, hop + 1))
                def _():
                    zg_copy(i, way, hop + 1).start()

            if hop > 0:

                @pl.when(can(way, hop))
                def _():
                    zg_copy(i, way, hop).wait_send()

    def on_bg(i):
        bg_copy(i).wait()
        gather(i, 0)

    def on_zg3(i):
        gather(i, 3)
        ag_copy(i).start()

    def on_ag(i):
        ag_copy(i).wait()
        dg_copy(i).start()

    def out_copy(i):
        m = (i > full).astype(jnp.int32)
        start = pl.multiple_of((i - m * (full + 1)) * W, W)
        return pltpu.make_async_copy(res.at[i], out_hbm.at[m, :, pl.ds(start, W)], out_sem.at[lax.rem(i, 4)])

    def out_mixed(i, m):
        part = pl.ds(m * (W // 2), W // 2)
        return pltpu.make_async_copy(res.at[i, :, part], out_hbm.at[m, :, pl.ds(full * W, W // 2)], out_sem.at[4 + m])

    def on_dg(i):
        dg_copy(i).wait()

        @pl.when(i != full)
        def _():
            out_copy(i).start()

        @pl.when(i == full)
        def _():
            out_mixed(i, 0).start()
            out_mixed(i, 1).start()

    def on_out(i):
        @pl.when(i != full)
        def _():
            out_copy(i).wait()

        @pl.when(i == full)
        def _():
            out_mixed(i, 0).wait()
            out_mixed(i, 1).wait()

    @pl.loop(0, chunks + O_OUT)
    def _(step):
        stage(step, 0, multiply)
        stage(step, O_D2D, on_d2d)
        stage(step, O_A, on_a)
        stage(step, O_Z1, on_z1)
        stage(step, O_Z2, on_z2)
        stage(step, O_Z3, on_z3)
        stage(step, O_B, on_b)
        stage(step, O_BG, on_bg)
        stage(step, O_ZG1, lambda i: gather(i, 1))
        stage(step, O_ZG2, lambda i: gather(i, 2))
        stage(step, O_ZG3, on_zg3)
        stage(step, O_AG, on_ag)
        stage(step, O_DG, on_dg)
        stage(step, O_OUT, on_out)


def solution(mesh):
    def step(a, g):
        _, mats, tokens, rows = a.shape
        cols = g.shape[-1]
        full = cols // W
        chunks = 2 * full + 1
        half, quarter, piece = rows // 2, rows // 4, rows // 32
        hbm = pl.BlockSpec(memory_space=pl.ANY)
        ring = lambda n: pltpu.VMEM((RING, n, W), BF16)
        return pl.pallas_call(
            functools.partial(kernel, full),
            out_shape=jax.ShapeDtypeStruct((mats, rows, cols), BF16),
            in_specs=[hbm, hbm],
            out_specs=hbm,
            scratch_shapes=[
                pltpu.VMEM((mats, tokens, rows), BF16),
                pltpu.VMEM((3, tokens, W), BF16),
                pltpu.VMEM((2, rows, W), F32),
                pltpu.VMEM((KEEP, quarter, W), F32),
                pltpu.VMEM((chunks, rows, W), BF16),
                ring(half),
                ring(half),
                *[ring(quarter)] * 6,
                ring(piece),
                ring(piece),
                pltpu.SemaphoreType.DMA((7,)),
                pltpu.SemaphoreType.DMA((6,)),
                pltpu.SemaphoreType.DMA((6, RING)),
                pltpu.SemaphoreType.DMA((6, RING)),
                pltpu.SemaphoreType.DMA((8, RING)),
                pltpu.SemaphoreType.DMA((8, RING)),
            ],
            compiler_params=pltpu.CompilerParams(
                collective_id=0, has_side_effects=True, vmem_limit_bytes=62 * 1024 * 1024
            ),
        )(a, g)

    return jax.shard_map(
        step, mesh=mesh, in_specs=(P(("rep", "dp")), P(("rep", "dp"))), out_specs=P("rep"), check_vma=False
    )
```

```python
import functools
import itertools

import jax
import jax.numpy as jnp
from jax import lax
from jax.experimental import pallas as pl
from jax.experimental.pallas import tpu as pltpu
from jax.sharding import PartitionSpec as P

W = 256
RING = 8
MESH = pl.DeviceIdType.MESH
F32, BF16 = jnp.float32, jnp.bfloat16

LAGS = dict(d2d=1, a=3, z1=3, z2=3, z3=3, b=3, zg1=3, zg2=3, zg3=5, ag=6, dg=2)
AT = dict(zip(LAGS, itertools.accumulate(LAGS.values())))
KEEP = (AT["b"] - AT["d2d"]) // 2 + 1


def kernel(full, a_hbm, g_hbm, res, a_v, g_v, acc, keep, d_send, d_recv, a_send, a_recv, zr_send, zr_recv, zl_send, zl_recv,
           b_send, b_recv, in_sem, s_sem, r_sem, zs_sem, zr_sem):
    chunks = 2 * full + 1
    rows = 2 * acc.shape[1]
    half, quarter, block = rows // 2, rows // 4, rows // 16
    me = lax.axis_index("dp")
    x, y, z, core = me // 16, (me // 8) % 2, (me // 2) % 4, me % 2

    def dev(x, y, z, core):
        return {"dp": ((x * 2 + y) * 4 + z) * 2 + core}

    partner = dev(x, y, z, 1 - core)
    first = 1 - core
    a_at = first * x + core * y
    a_dev = dev(x + first * (1 - 2 * x), y + core * (1 - 2 * y), z, core)
    b_dev = dev(x + core * (1 - 2 * x), y + first * (1 - 2 * y), z, core)
    right, left = dev(x, y, z + 1, core), dev(x, y, z - 1, core)

    def at(start, size):
        return pl.ds(pl.multiple_of(start, size), size)

    def remote(src, dst, send, recv, to):
        return pltpu.make_async_remote_copy(src, dst, send, recv, device_id=to, device_id_type=MESH)

    def g_copies(i, slot):
        m = (i > full).astype(jnp.int32)
        start = pl.multiple_of((i - m * (full + 1)) * W, W)
        return pltpu.make_async_copy(g_hbm.at[0, m, :, pl.ds(start, W)], g_v.at[slot], in_sem.at[slot])

    def g_mixed(m, slot):
        return pltpu.make_async_copy(
            g_hbm.at[0, m, :, pl.ds(full * W, W // 2)], g_v.at[slot, :, pl.ds(m * (W // 2), W // 2)], in_sem.at[3 + m]
        )

    def g_start(i, slot):
        @pl.when(i != full)
        def _():
            g_copies(i, slot).start()

        @pl.when(i == full)
        def _():
            g_mixed(0, slot).start()
            g_mixed(1, slot).start()

    def a_copy(m):
        return pltpu.make_async_copy(a_hbm.at[0, m], a_v.at[m], in_sem.at[5 + m])

    a_copy(0).start()
    for i in range(3):
        g_start(jnp.int32(i), i)
    a_copy(1).start()

    barrier = pltpu.get_barrier_semaphore()
    for to in (partner, a_dev, b_dev):
        pl.semaphore_signal(barrier, inc=1, device_id=to, device_id_type=MESH)

    @pl.when(z < 3)
    def _():
        pl.semaphore_signal(barrier, inc=1, device_id=right, device_id_type=MESH)

    @pl.when(z > 0)
    def _():
        pl.semaphore_signal(barrier, inc=1, device_id=left, device_id_type=MESH)

    pl.semaphore_wait(barrier, 3 + (z < 3).astype(jnp.int32) + (z > 0).astype(jnp.int32))
    a_copy(0).wait()

    def pair(k, i, src, dst, to):
        s = lax.rem(i, RING)
        return remote(src, dst, s_sem.at[k, s], r_sem.at[k, s], to)

    def d_copy(i):
        s = lax.rem(i, RING)
        return pair(0, i, d_send.at[s], d_recv.at[s], partner)

    def a_copy_out(i):
        s = lax.rem(i, RING)
        return pair(1, i, a_send.at[s], a_recv.at[s], a_dev)

    def b_copy(i):
        s = lax.rem(i, RING)
        return pair(2, i, b_send.at[s], b_recv.at[s], b_dev)

    mine_a = core * half + a_at * quarter
    mine_z = mine_a + z * block

    def ag_copy(i):
        ref = res.at[i, at(mine_a, quarter)]
        return pair(3, i, ref, ref, a_dev)

    def dg_copy(i):
        ref = res.at[i, at(core * half, half)]
        return pair(4, i, ref, ref, partner)

    def z_copy(i, way, lo, hi):
        s = lax.rem(i, RING)
        send, recv, to = ((zr_send, zr_recv, right), (zl_send, zl_recv, left))[way]
        there = pl.ds(lo * block, (hi - lo) * block)
        return remote(send.at[s, there], recv.at[s, there], zs_sem.at[way, s], zr_sem.at[way, s], to)

    def zg_copy(i, way, hop):
        s = lax.rem(i, RING)
        owner = z - (hop - 1) if way == 0 else z + (hop - 1)
        ref = res.at[i, at(mine_a + owner * block, block)]
        k = 2 + way * 3 + hop - 1
        return remote(ref, ref, zs_sem.at[k, s], zr_sem.at[k, s], (right, left)[way])

    def stage(step, part, name, body):
        if AT[name] % 2 == part:
            i = step - AT[name] // 2

            @pl.when((i >= 0) & (i < chunks))
            def _():
                body(i)

    def product(i, slot, cols, put):
        dims = (((0,), (0,)), ((), ()))

        @pl.when(i != full)
        def _():
            m = (i > full).astype(jnp.int32)
            put(pl.ds(0, W), lax.dot_general(a_v[m, :, cols], g_v[slot], dims, preferred_element_type=F32))

        @pl.when(i == full)
        def _():
            for m in range(2):
                part = pl.ds(m * (W // 2), W // 2)
                put(part, lax.dot_general(a_v[m, :, cols], g_v[slot, :, part], dims, preferred_element_type=F32))

    def multiply_other(i):
        slot = lax.rem(i, 3)
        s = lax.rem(i, RING)

        @pl.when(i != full)
        def _():
            g_copies(i, slot).wait()

        @pl.when(i == full)
        def _():
            a_copy(1).wait()
            g_mixed(0, slot).wait()
            g_mixed(1, slot).wait()

        def put(part, sums):
            d_send[s, :, part] = sums.astype(BF16)

        product(i, slot, at((1 - core) * half, half), put)
        d_copy(i).start()

    def multiply_mine(i):
        slot = lax.rem(i, 3)
        now = lax.rem(i, 2)

        def put(part, sums):
            acc[now, :, part] = sums

        product(i, slot, at(core * half, half), put)

        @pl.when(i + 3 < chunks)
        def _():
            g_start(i + 3, slot)

    def on_d2d(i):
        d_copy(i).wait()
        s, k, now = lax.rem(i, RING), lax.rem(i, KEEP), lax.rem(i, 2)

        def total(which):
            here = at(which * quarter, quarter)
            return acc[now, here] + d_recv[s, here].astype(F32)

        a_send[s] = total(1 - a_at).astype(BF16)
        a_copy_out(i).start()
        keep[k] = total(a_at)

    def on_a(i):
        a_copy_out(i).wait()
        s, k = lax.rem(i, RING), lax.rem(i, KEEP)
        keep[k] += a_recv[s].astype(F32)

        @pl.when(z == 0)
        def _():
            there = pl.ds(block, 3 * block)
            zr_send[s, there] = keep[k, there].astype(BF16)
            z_copy(i, 0, 1, 4).start()

        @pl.when(z == 3)
        def _():
            there = pl.ds(0, 3 * block)
            zl_send[s, there] = keep[k, there].astype(BF16)
            z_copy(i, 1, 0, 3).start()

    def pass_on(i, way, at_z):
        s, k = lax.rem(i, RING), lax.rem(i, KEEP)
        send, recv = ((zr_send, zr_recv), (zl_send, zl_recv))[way]
        lo, hi = ((at_z, 4), (0, at_z + 1))[way]

        @pl.when(z == at_z)
        def _():
            z_copy(i, way, lo, hi).wait_recv()
            lo2, hi2 = ((at_z + 1, 4), (0, at_z))[way]
            if lo2 < hi2:
                beyond = pl.ds(lo2 * block, (hi2 - lo2) * block)
                send[s, beyond] = (keep[k, beyond] + recv[s, beyond].astype(F32)).astype(BF16)
                z_copy(i, way, lo2, hi2).start()
            here = pl.ds(at_z * block, block)
            keep[k, here] += recv[s, here].astype(F32)

    def sent(i, way, at_z):
        lo, hi = ((at_z + 1, 4), (0, at_z))[way]

        @pl.when(z == at_z)
        def _():
            z_copy(i, way, lo, hi).wait_send()

    def on_z1(i):
        sent(i, 0, 0)
        sent(i, 1, 3)
        pass_on(i, 0, 1)
        pass_on(i, 1, 2)

    def on_z2(i):
        sent(i, 0, 1)
        sent(i, 1, 2)
        pass_on(i, 0, 2)
        pass_on(i, 1, 1)

    def on_z3(i):
        sent(i, 0, 2)
        sent(i, 1, 1)
        pass_on(i, 0, 3)
        pass_on(i, 1, 0)
        s, k = lax.rem(i, RING), lax.rem(i, KEEP)
        b_send[s] = keep[k, at(z * block, block)].astype(BF16)
        b_copy(i).start()

    def on_b(i):
        b_copy(i).wait()
        s = lax.rem(i, RING)
        total = b_send[s].astype(F32) + b_recv[s].astype(F32)
        res[i, at(mine_z, block)] = total.astype(BF16)
        gather(i, 0)

    def can(way, hop):
        return (z >= hop - 1) & (z < 3) if way == 0 else (z <= 4 - hop) & (z > 0)

    def gets(way, hop):
        return z >= hop if way == 0 else z <= 3 - hop

    def gather(i, hop):
        for way in range(2):
            if hop > 0:

                @pl.when(gets(way, hop))
                def _():
                    zg_copy(i, way, hop).wait_recv()

            if hop < 3:

                @pl.when(can(way, hop + 1))
                def _():
                    zg_copy(i, way, hop + 1).start()

            if hop > 0:

                @pl.when(can(way, hop))
                def _():
                    zg_copy(i, way, hop).wait_send()

    def on_zg3(i):
        gather(i, 3)
        ag_copy(i).start()

    def on_ag(i):
        ag_copy(i).wait()
        dg_copy(i).start()

    def on_dg(i):
        dg_copy(i).wait()

    @pl.loop(0, chunks + (AT["dg"] + 1) // 2)
    def _(step):
        for part in range(2):

            @pl.when(step < chunks)
            def _():
                (multiply_other, multiply_mine)[part](step)

            stage(step, part, "d2d", on_d2d)
            stage(step, part, "a", on_a)
            stage(step, part, "z1", on_z1)
            stage(step, part, "z2", on_z2)
            stage(step, part, "z3", on_z3)
            stage(step, part, "b", on_b)
            stage(step, part, "zg1", lambda i: gather(i, 1))
            stage(step, part, "zg2", lambda i: gather(i, 2))
            stage(step, part, "zg3", on_zg3)
            stage(step, part, "ag", on_ag)
            stage(step, part, "dg", on_dg)


def place(full, blocks, out, sem):
    chunks = 2 * full + 1
    copies = []
    for m in range(2):
        for j in range(full):
            i = m * (full + 1) + j
            copies.append(pltpu.make_async_copy(blocks.at[i], out.at[m, :, pl.ds(j * W, W)], sem.at[i]))
        part = pl.ds(m * (W // 2), W // 2)
        copies.append(
            pltpu.make_async_copy(blocks.at[full, :, part], out.at[m, :, pl.ds(full * W, W // 2)], sem.at[full + m * (full + 1)])
        )
    for c in copies:
        c.start()
    for c in copies:
        c.wait()


def solution(mesh):
    def step(a, g):
        _, mats, tokens, rows = a.shape
        cols = g.shape[-1]
        full = cols // W
        chunks = 2 * full + 1
        half, quarter, block = rows // 2, rows // 4, rows // 16
        hbm = pl.BlockSpec(memory_space=pl.ANY)
        ring = lambda n: pltpu.VMEM((RING, n, W), BF16)
        blocks = pl.pallas_call(
            functools.partial(kernel, full),
            out_shape=pltpu.VMEM((chunks, rows, W), BF16),
            in_specs=[hbm, hbm],
            out_specs=pl.BlockSpec(memory_space=pltpu.VMEM),
            scratch_shapes=[
                pltpu.VMEM((mats, tokens, rows), BF16),
                pltpu.VMEM((3, tokens, W), BF16),
                pltpu.VMEM((2, half, W), F32),
                pltpu.VMEM((KEEP, quarter, W), F32),
                ring(half),
                ring(half),
                *[ring(quarter)] * 6,
                ring(block),
                ring(block),
                pltpu.SemaphoreType.DMA((7,)),
                pltpu.SemaphoreType.DMA((5, RING)),
                pltpu.SemaphoreType.DMA((5, RING)),
                pltpu.SemaphoreType.DMA((8, RING)),
                pltpu.SemaphoreType.DMA((8, RING)),
            ],
            compiler_params=pltpu.CompilerParams(
                collective_id=0, has_side_effects=True, vmem_limit_bytes=48 * 1024 * 1024
            ),
        )(a, g)
        return pl.pallas_call(
            functools.partial(place, full),
            out_shape=jax.ShapeDtypeStruct((mats, rows, cols), BF16),
            in_specs=[pl.BlockSpec(memory_space=pltpu.VMEM)],
            out_specs=hbm,
            scratch_shapes=[pltpu.SemaphoreType.DMA((chunks + 1,))],
            compiler_params=pltpu.CompilerParams(vmem_limit_bytes=16 * 1024 * 1024),
        )(blocks)

    return jax.shard_map(
        step, mesh=mesh, in_specs=(P(("rep", "dp")), P(("rep", "dp"))), out_specs=P("rep"), check_vma=False
    )
```

```python
import functools
import itertools

import jax
import jax.numpy as jnp
from jax import lax
from jax.experimental import pallas as pl
from jax.experimental.pallas import tpu as pltpu
from jax.sharding import PartitionSpec as P

W = 256
RING = 8
MESH = pl.DeviceIdType.MESH
F32, BF16 = jnp.float32, jnp.bfloat16

LAGS = dict(d2d=1, a=3, z1=3, z2=3, z3=3, b=3, zg1=3, zg2=3, zg3=5, ag=6, dg=2)
AT = dict(zip(LAGS, itertools.accumulate(LAGS.values())))
KEEP = (AT["b"] - AT["d2d"]) // 2 + 1


def kernel(full, a_hbm, g_hbm, res, a_v, g_v, acc, keep, d_send, d_recv, a_send, a_recv, zr_send, zr_recv, zl_send, zl_recv,
           b_send, b_recv, in_sem, s_sem, r_sem, zs_sem, zr_sem):
    chunks = 2 * full + 1
    rows = 2 * acc.shape[1]
    half, quarter, block = rows // 2, rows // 4, rows // 16
    me = lax.axis_index("dp")
    x, y, z, core = me // 16, (me // 8) % 2, (me // 2) % 4, me % 2

    def dev(x, y, z, core):
        return {"dp": ((x * 2 + y) * 4 + z) * 2 + core}

    partner = dev(x, y, z, 1 - core)
    first = 1 - core
    a_at = first * x + core * y
    a_dev = dev(x + first * (1 - 2 * x), y + core * (1 - 2 * y), z, core)
    b_dev = dev(x + core * (1 - 2 * x), y + first * (1 - 2 * y), z, core)
    right, left = dev(x, y, z + 1, core), dev(x, y, z - 1, core)

    def at(start, size):
        return pl.ds(pl.multiple_of(start, size), size)

    def remote(src, dst, send, recv, to):
        return pltpu.make_async_remote_copy(src, dst, send, recv, device_id=to, device_id_type=MESH)

    def g_copies(i, slot):
        m = (i > full).astype(jnp.int32)
        start = pl.multiple_of((i - m * (full + 1)) * W, W)
        return pltpu.make_async_copy(g_hbm.at[0, m, :, pl.ds(start, W)], g_v.at[slot], in_sem.at[slot])

    def g_mixed(m, slot):
        return pltpu.make_async_copy(
            g_hbm.at[0, m, :, pl.ds(full * W, W // 2)], g_v.at[slot, :, pl.ds(m * (W // 2), W // 2)], in_sem.at[3 + m]
        )

    def g_start(i, slot):
        @pl.when(i != full)
        def _():
            g_copies(i, slot).start()

        @pl.when(i == full)
        def _():
            g_mixed(0, slot).start()
            g_mixed(1, slot).start()

    other_cols, my_cols = at((1 - core) * half, half), at(core * half, half)

    def a_copy(m, cols, k):
        return pltpu.make_async_copy(a_hbm.at[0, m, :, cols], a_v.at[m, :, cols], in_sem.at[5 + 2 * m + k])

    a_copy(0, other_cols, 0).start()
    g_start(jnp.int32(0), 0)

    barrier = pltpu.get_barrier_semaphore()
    for to in (partner, a_dev, b_dev):
        pl.semaphore_signal(barrier, inc=1, device_id=to, device_id_type=MESH)

    @pl.when(z < 3)
    def _():
        pl.semaphore_signal(barrier, inc=1, device_id=right, device_id_type=MESH)

    @pl.when(z > 0)
    def _():
        pl.semaphore_signal(barrier, inc=1, device_id=left, device_id_type=MESH)

    pl.semaphore_wait(barrier, 3 + (z < 3).astype(jnp.int32) + (z > 0).astype(jnp.int32))
    a_copy(0, my_cols, 1).start()
    g_start(jnp.int32(1), 1)
    g_start(jnp.int32(2), 2)
    a_copy(0, other_cols, 0).wait()

    def pair(k, i, src, dst, to):
        s = lax.rem(i, RING)
        return remote(src, dst, s_sem.at[k, s], r_sem.at[k, s], to)

    def d_copy(i):
        s = lax.rem(i, RING)
        return pair(0, i, d_send.at[s], d_recv.at[s], partner)

    def a_copy_out(i):
        s = lax.rem(i, RING)
        return pair(1, i, a_send.at[s], a_recv.at[s], a_dev)

    def b_copy(i):
        s = lax.rem(i, RING)
        return pair(2, i, b_send.at[s], b_recv.at[s], b_dev)

    mine_a = core * half + a_at * quarter
    mine_z = mine_a + z * block

    def ag_copy(i):
        ref = res.at[i, at(mine_a, quarter)]
        return pair(3, i, ref, ref, a_dev)

    def dg_copy(i):
        ref = res.at[i, at(core * half, half)]
        return pair(4, i, ref, ref, partner)

    def z_copy(i, way, lo, hi):
        s = lax.rem(i, RING)
        send, recv, to = ((zr_send, zr_recv, right), (zl_send, zl_recv, left))[way]
        there = pl.ds(lo * block, (hi - lo) * block)
        return remote(send.at[s, there], recv.at[s, there], zs_sem.at[way, s], zr_sem.at[way, s], to)

    def zg_copy(i, way, hop):
        s = lax.rem(i, RING)
        owner = z - (hop - 1) if way == 0 else z + (hop - 1)
        ref = res.at[i, at(mine_a + owner * block, block)]
        k = 2 + way * 3 + hop - 1
        return remote(ref, ref, zs_sem.at[k, s], zr_sem.at[k, s], (right, left)[way])

    def stage(step, part, name, body):
        if AT[name] % 2 == part:
            i = step - AT[name] // 2

            @pl.when((i >= 0) & (i < chunks))
            def _():
                body(i)

    def product(i, slot, cols, put):
        dims = (((0,), (0,)), ((), ()))

        @pl.when(i != full)
        def _():
            m = (i > full).astype(jnp.int32)
            put(pl.ds(0, W), lax.dot_general(a_v[m, :, cols], g_v[slot], dims, preferred_element_type=F32))

        @pl.when(i == full)
        def _():
            for m in range(2):
                part = pl.ds(m * (W // 2), W // 2)
                put(part, lax.dot_general(g_v[slot, :, part], a_v[m, :, cols], dims, preferred_element_type=F32).T)

    def multiply_other(i):
        slot = lax.rem(i, 3)
        s = lax.rem(i, RING)

        @pl.when(i != full)
        def _():
            g_copies(i, slot).wait()

        @pl.when(i == full)
        def _():
            a_copy(1, other_cols, 0).wait()
            a_copy(1, my_cols, 1).wait()
            g_mixed(0, slot).wait()
            g_mixed(1, slot).wait()

        def put(part, sums):
            d_send[s, :, part] = sums.astype(BF16)

        product(i, slot, other_cols, put)
        d_copy(i).start()

    def multiply_mine(i):
        slot = lax.rem(i, 3)
        now = lax.rem(i, 2)

        def put(part, sums):
            acc[now, :, part] = sums

        @pl.when(i == 0)
        def _():
            a_copy(0, my_cols, 1).wait()

        @pl.when(i == 1)
        def _():
            a_copy(1, other_cols, 0).start()
            a_copy(1, my_cols, 1).start()

        product(i, slot, my_cols, put)

        @pl.when(i + 3 < chunks)
        def _():
            g_start(i + 3, slot)

    def on_d2d(i):
        d_copy(i).wait()
        s, k, now = lax.rem(i, RING), lax.rem(i, KEEP), lax.rem(i, 2)

        def total(which):
            here = at(which * quarter, quarter)
            return acc[now, here] + d_recv[s, here].astype(F32)

        a_send[s] = total(1 - a_at).astype(BF16)
        a_copy_out(i).start()
        keep[k] = total(a_at)

    def on_a(i):
        a_copy_out(i).wait()
        s, k = lax.rem(i, RING), lax.rem(i, KEEP)
        keep[k] += a_recv[s].astype(F32)

        @pl.when(z == 0)
        def _():
            there = pl.ds(block, 3 * block)
            zr_send[s, there] = keep[k, there].astype(BF16)
            z_copy(i, 0, 1, 4).start()

        @pl.when(z == 3)
        def _():
            there = pl.ds(0, 3 * block)
            zl_send[s, there] = keep[k, there].astype(BF16)
            z_copy(i, 1, 0, 3).start()

    def pass_on(i, way, at_z):
        s, k = lax.rem(i, RING), lax.rem(i, KEEP)
        send, recv = ((zr_send, zr_recv), (zl_send, zl_recv))[way]
        lo, hi = ((at_z, 4), (0, at_z + 1))[way]

        @pl.when(z == at_z)
        def _():
            z_copy(i, way, lo, hi).wait_recv()
            lo2, hi2 = ((at_z + 1, 4), (0, at_z))[way]
            if lo2 < hi2:
                beyond = pl.ds(lo2 * block, (hi2 - lo2) * block)
                send[s, beyond] = (keep[k, beyond] + recv[s, beyond].astype(F32)).astype(BF16)
                z_copy(i, way, lo2, hi2).start()
            here = pl.ds(at_z * block, block)
            keep[k, here] += recv[s, here].astype(F32)

    def sent(i, way, at_z):
        lo, hi = ((at_z + 1, 4), (0, at_z))[way]

        @pl.when(z == at_z)
        def _():
            z_copy(i, way, lo, hi).wait_send()

    def on_z1(i):
        sent(i, 0, 0)
        sent(i, 1, 3)
        pass_on(i, 0, 1)
        pass_on(i, 1, 2)

    def on_z2(i):
        sent(i, 0, 1)
        sent(i, 1, 2)
        pass_on(i, 0, 2)
        pass_on(i, 1, 1)

    def on_z3(i):
        sent(i, 0, 2)
        sent(i, 1, 1)
        pass_on(i, 0, 3)
        pass_on(i, 1, 0)
        s, k = lax.rem(i, RING), lax.rem(i, KEEP)
        b_send[s] = keep[k, at(z * block, block)].astype(BF16)
        b_copy(i).start()

    def on_b(i):
        b_copy(i).wait()
        s = lax.rem(i, RING)
        total = b_send[s].astype(F32) + b_recv[s].astype(F32)
        res[i, at(mine_z, block)] = total.astype(BF16)
        gather(i, 0)

    def can(way, hop):
        return (z >= hop - 1) & (z < 3) if way == 0 else (z <= 4 - hop) & (z > 0)

    def gets(way, hop):
        return z >= hop if way == 0 else z <= 3 - hop

    def gather(i, hop):
        for way in range(2):
            if hop > 0:

                @pl.when(gets(way, hop))
                def _():
                    zg_copy(i, way, hop).wait_recv()

            if hop < 3:

                @pl.when(can(way, hop + 1))
                def _():
                    zg_copy(i, way, hop + 1).start()

            if hop > 0:

                @pl.when(can(way, hop))
                def _():
                    zg_copy(i, way, hop).wait_send()

    def on_zg3(i):
        gather(i, 3)
        ag_copy(i).start()

    def on_ag(i):
        ag_copy(i).wait()
        dg_copy(i).start()

    def on_dg(i):
        dg_copy(i).wait()

    @pl.loop(0, chunks + (AT["dg"] + 1) // 2)
    def _(step):
        for part in range(2):

            @pl.when(step < chunks)
            def _():
                (multiply_other, multiply_mine)[part](step)

            stage(step, part, "d2d", on_d2d)
            stage(step, part, "a", on_a)
            stage(step, part, "z1", on_z1)
            stage(step, part, "z2", on_z2)
            stage(step, part, "z3", on_z3)
            stage(step, part, "b", on_b)
            stage(step, part, "zg1", lambda i: gather(i, 1))
            stage(step, part, "zg2", lambda i: gather(i, 2))
            stage(step, part, "zg3", on_zg3)
            stage(step, part, "ag", on_ag)
            stage(step, part, "dg", on_dg)


def place(full, blocks, out, sem):
    chunks = 2 * full + 1
    copies = []
    for m in range(2):
        for j in range(full):
            i = m * (full + 1) + j
            copies.append(pltpu.make_async_copy(blocks.at[i], out.at[m, :, pl.ds(j * W, W)], sem.at[i]))
        part = pl.ds(m * (W // 2), W // 2)
        copies.append(
            pltpu.make_async_copy(blocks.at[full, :, part], out.at[m, :, pl.ds(full * W, W // 2)], sem.at[full + m * (full + 1)])
        )
    for c in copies:
        c.start()
    for c in copies:
        c.wait()


def solution(mesh):
    def step(a, g):
        _, mats, tokens, rows = a.shape
        cols = g.shape[-1]
        full = cols // W
        chunks = 2 * full + 1
        half, quarter, block = rows // 2, rows // 4, rows // 16
        hbm = pl.BlockSpec(memory_space=pl.ANY)
        ring = lambda n: pltpu.VMEM((RING, n, W), BF16)
        blocks = pl.pallas_call(
            functools.partial(kernel, full),
            out_shape=pltpu.VMEM((chunks, rows, W), BF16),
            in_specs=[hbm, hbm],
            out_specs=pl.BlockSpec(memory_space=pltpu.VMEM),
            scratch_shapes=[
                pltpu.VMEM((mats, tokens, rows), BF16),
                pltpu.VMEM((3, tokens, W), BF16),
                pltpu.VMEM((2, half, W), F32),
                pltpu.VMEM((KEEP, quarter, W), F32),
                ring(half),
                ring(half),
                *[ring(quarter)] * 6,
                ring(block),
                ring(block),
                pltpu.SemaphoreType.DMA((9,)),
                pltpu.SemaphoreType.DMA((5, RING)),
                pltpu.SemaphoreType.DMA((5, RING)),
                pltpu.SemaphoreType.DMA((8, RING)),
                pltpu.SemaphoreType.DMA((8, RING)),
            ],
            compiler_params=pltpu.CompilerParams(
                collective_id=0, has_side_effects=True, vmem_limit_bytes=48 * 1024 * 1024
            ),
        )(a, g)
        return pl.pallas_call(
            functools.partial(place, full),
            out_shape=jax.ShapeDtypeStruct((mats, rows, cols), BF16),
            in_specs=[pl.BlockSpec(memory_space=pltpu.VMEM)],
            out_specs=hbm,
            scratch_shapes=[pltpu.SemaphoreType.DMA((chunks + 1,))],
            compiler_params=pltpu.CompilerParams(vmem_limit_bytes=16 * 1024 * 1024),
        )(blocks)

    return jax.shard_map(
        step, mesh=mesh, in_specs=(P(("rep", "dp")), P(("rep", "dp"))), out_specs=P("rep"), check_vma=False
    )
```
